8 devices in a mesh: data: 8 (over z, y, x, core).
Axes of the slice: x: 2, y: 2, z: 1, core: 2. Of those that a mesh axis runs over, the one named last changes fastest.
Arguments:
- grad_attn: bfloat16 [8, 12, 1048576], P('data')
- grad_mlp: bfloat16 [8, 6, 4194304], P('data')
- grad_wide: bfloat16 [8, 3, 4096], P('data')
- grad_vec: bfloat16 [8, 29, 1024], P('data')
- weight_attn: float32 [12, 1048576], P(None, 'data')
- weight_mlp: float32 [6, 4194304], P(None, 'data')
- weight_wide: float32 [3, 4096], P(None, 'data')
- weight_vec: float32 [29, 1024], P(None, 'data')
- mom1_attn: float32 [12, 1048576], P(None, 'data')
- mom1_mlp: float32 [6, 4194304], P(None, 'data')
- mom1_wide: float32 [3, 4096], P(None, 'data')
- mom1_vec: float32 [29, 1024], P(None, 'data')
- mom2_attn: float32 [12, 1048576], P(None, 'data')
- mom2_mlp: float32 [6, 4194304], P(None, 'data')
- mom2_wide: float32 [3, 4096], P(None, 'data')
- mom2_vec: float32 [29, 1024], P(None, 'data')
Outputs:
- output 1: bfloat16 [12, 1048576], replicated
- output 2: bfloat16 [6, 4194304], replicated
- output 3: bfloat16 [3, 4096], replicated
- output 4: bfloat16 [29, 1024], replicated
- output 5: float32 [12, 1048576], P(None, 'data')
- output 6: float32 [6, 4194304], P(None, 'data')
- output 7: float32 [3, 4096], P(None, 'data')
- output 8: float32 [29, 1024], P(None, 'data')
- output 9: float32 [12, 1048576], P(None, 'data')
- output 10: float32 [6, 4194304], P(None, 'data')
- output 11: float32 [3, 4096], P(None, 'data')
- output 12: float32 [29, 1024], P(None, 'data')
- output 13: float32 [12, 1048576], P(None, 'data')
- output 14: float32 [6, 4194304], P(None, 'data')
- output 15: float32 [3, 4096], P(None, 'data')
- output 16: float32 [29, 1024], P(None, 'data')
All inputs are finite; a program needn't handle non-finite values.
Results may differ from the reference program's by a relative error of at most 0.001.
Values are sent between devices in bfloat16 or wider.
A program may use at most 1 GiB of HBM per device.

```python
import jax
import jax.numpy as jnp

GROUP_SIZE = 8
LAYERS = 3
D = 1024
FF = 4096
STEP_NUMBER = 10

LEARN_RATE = 0.04
BETA_FIRST = 0.9
BETA_SECOND = 0.999
EPSILON = 1e-6
WEIGHT_DECAY = 0.01
MAX_NORM = 1.0
TARGET_NORM = 3.0


def bank_layout():
    gain_rows = jnp.array([1.0, 0.0, 0.0, 0.0, 0.0, 0.0, 1.0, 0.0, 0.0] * LAYERS + [1.0, 0.0])
    counts = (4 * LAYERS, 2 * LAYERS, LAYERS, 9 * LAYERS + 2)
    lengths = (D * D, D * FF, FF, D)
    base_scales = (
        jnp.full((4 * LAYERS,), D ** -0.5),
        jnp.array([D ** -0.5, FF ** -0.5] * LAYERS),
        jnp.full((LAYERS,), 0.05),
        0.05 + 0.15 * gain_rows,
    )
    offsets = (jnp.zeros((4 * LAYERS,)), jnp.zeros((2 * LAYERS,)), jnp.zeros((LAYERS,)), gain_rows)
    return counts, lengths, base_scales, offsets


def setup_inputs(seed: int = 0) -> dict:
    root_key = jax.random.key(seed)
    counts, lengths, base_scales, offsets = bank_layout()
    bank_keys = [jax.random.split(jax.random.fold_in(root_key, bank_index), 6) for bank_index in range(4)]
    grad_mults = [jnp.exp(jax.random.uniform(bank_keys[bank_index][0], (counts[bank_index],), minval=-1.0, maxval=1.0)) for bank_index in range(4)]
    weighted = sum(lengths[bank_index] * jnp.sum(grad_mults[bank_index] ** 2) for bank_index in range(4))
    grad_unit = TARGET_NORM * jnp.sqrt(GROUP_SIZE / weighted)
    clip_guess = MAX_NORM / TARGET_NORM
    grad_banks, weights, firsts, seconds = [], [], [], []
    for bank_index in range(4):
        bank_keyset = bank_keys[bank_index]
        row_count = counts[bank_index]
        row_length = lengths[bank_index]
        grad_scale = grad_unit * grad_mults[bank_index]
        device_grads = jax.random.normal(bank_keyset[1], (GROUP_SIZE, row_count, row_length)) * grad_scale[None, :, None]
        grad_banks.append(device_grads.astype(jnp.bfloat16))
        weight_spread = jnp.exp(jax.random.uniform(bank_keyset[2], (row_count,), minval=-1.2, maxval=1.2))
        row_scale = base_scales[bank_index] * weight_spread
        weights.append(offsets[bank_index][:, None] + row_scale[:, None] * jax.random.normal(bank_keyset[3], (row_count, row_length)))
        moment_unit = clip_guess * grad_scale / GROUP_SIZE ** 0.5
        firsts.append(0.1 * moment_unit[:, None] * jax.random.normal(bank_keyset[4], (row_count, row_length)))
        seconds.append(0.001 * (moment_unit * moment_unit)[:, None] * jnp.exp(0.5 * jax.random.normal(bank_keyset[5], (row_count, row_length))))
    bank_names = ("attn", "mlp", "wide", "vec")
    inputs = {}
    for prefix, arrays in (("grad_", grad_banks), ("weight_", weights), ("mom1_", firsts), ("mom2_", seconds)):
        for bank_index in range(4):
            inputs[prefix + bank_names[bank_index]] = arrays[bank_index]
    return inputs


def lamb_bank(mean_grad, weight, first_moment, second_moment, clip_coef):
    clipped = clip_coef * mean_grad
    new_first = BETA_FIRST * first_moment + (1.0 - BETA_FIRST) * clipped
    new_second = BETA_SECOND * second_moment + (1.0 - BETA_SECOND) * (clipped * clipped)
    update = (new_first / (1.0 - BETA_FIRST ** STEP_NUMBER)) / (jnp.sqrt(new_second / (1.0 - BETA_SECOND ** STEP_NUMBER)) + EPSILON) + WEIGHT_DECAY * weight
    weight_norm = jnp.sqrt(jnp.sum(weight * weight, axis=1, keepdims=True))
    update_norm = jnp.sqrt(jnp.sum(update * update, axis=1, keepdims=True))
    new_weight = weight - LEARN_RATE * (weight_norm / update_norm) * update
    return new_weight.astype(jnp.bfloat16), new_weight, new_first, new_second


def reference(grad_attn, grad_mlp, grad_wide, grad_vec, weight_attn, weight_mlp, weight_wide, weight_vec, mom1_attn, mom1_mlp, mom1_wide, mom1_vec, mom2_attn, mom2_mlp, mom2_wide, mom2_vec):
    mean_attn = jnp.sum(grad_attn, axis=0, dtype=jnp.float32) / GROUP_SIZE
    mean_mlp = jnp.sum(grad_mlp, axis=0, dtype=jnp.float32) / GROUP_SIZE
    mean_wide = jnp.sum(grad_wide, axis=0, dtype=jnp.float32) / GROUP_SIZE
    mean_vec = jnp.sum(grad_vec, axis=0, dtype=jnp.float32) / GROUP_SIZE
    total_square = jnp.sum(mean_attn * mean_attn) + jnp.sum(mean_mlp * mean_mlp) + jnp.sum(mean_wide * mean_wide) + jnp.sum(mean_vec * mean_vec)
    clip_coef = jnp.minimum(1.0, MAX_NORM / jnp.sqrt(total_square))
    attn_out = lamb_bank(mean_attn, weight_attn, mom1_attn, mom2_attn, clip_coef)
    mlp_out = lamb_bank(mean_mlp, weight_mlp, mom1_mlp, mom2_mlp, clip_coef)
    wide_out = lamb_bank(mean_wide, weight_wide, mom1_wide, mom2_wide, clip_coef)
    vec_out = lamb_bank(mean_vec, weight_vec, mom1_vec, mom2_vec, clip_coef)
    return (attn_out[0], mlp_out[0], wide_out[0], vec_out[0], attn_out[1], mlp_out[1], wide_out[1], vec_out[1], attn_out[2], mlp_out[2], wide_out[2], vec_out[2], attn_out[3], mlp_out[3], wide_out[3], vec_out[3])
```

```python
import functools

import jax
import jax.numpy as jnp
from jax import lax
from jax.experimental import pallas as pl
from jax.experimental.pallas import tpu as pltpu
from jax.sharding import PartitionSpec as P

STEP_NUMBER = 10
LEARN_RATE = 0.04
BETA_FIRST = 0.9
BETA_SECOND = 0.999
EPSILON = 1e-6
WEIGHT_DECAY = 0.01
MAX_NORM = 1.0

MESH = pl.DeviceIdType.MESH
SLOTS = 8
AHEAD = 2
LAG_ONE = 4
LAG_TWO = 8
ATTN_WIDTH = 1024


def signal_all_and_wait(me, devices):
    barrier = pltpu.get_barrier_semaphore()
    for step in range(1, devices):
        pl.semaphore_signal(barrier, inc=1, device_id=(lax.rem(me + step, devices),), device_id_type=MESH)
    pl.semaphore_wait(barrier, devices - 1)


def share_tile(me, devices, tiles, send_sem, recv_sem):
    copies = []
    for step in range(1, devices):
        other = lax.rem(me + step, devices)
        copy = pltpu.make_async_remote_copy(
            src_ref=tiles.at[me], dst_ref=tiles.at[me], send_sem=send_sem.at[step], recv_sem=recv_sem.at[step],
            device_id=(other,), device_id_type=MESH)
        copy.start()
        copies.append(copy)
    for copy in copies:
        copy.wait()


def scatter_kernel(devices, widths, chunks, ga, gm, gw, gv, oa, om, ow, ov, total,
                   la, lm, pa, pm, s1a, s1m, r1a, r1m, s2a, s2m, r2a, r2m, ba, bm, rw, rv, sqa, sqm, tiles,
                   load_sem, psend_sem, precv_sem, send1_sem, recv1_sem, send2_sem, recv2_sem, out_sem,
                   wsend_sem, wrecv_sem, vsend_sem, vrecv_sem, tsend_sem, trecv_sem, pcredit, credit1, credit2):
    me = lax.axis_index("data")
    core = lax.rem(me, 2)
    x = lax.rem(me // 2, 2)
    y = me // 4
    partner = me + 1 - 2 * core
    xn = y * 4 + (1 - x) * 2 + core
    yn = (1 - y) * 4 + x * 2 + core
    banks = ((ga, oa, la, pa, s1a, r1a, s2a, r2a, ba, sqa, widths[0]), (gm, om, lm, pm, s1m, r1m, s2m, r2m, bm, sqm, widths[1]))

    signal_all_and_wait(me, devices)

    small = []
    for step in range(1, devices):
        other = lax.rem(me + step, devices)
        for src, dst, ssem, rsem in ((gw, rw, wsend_sem, wrecv_sem), (gv, rv, vsend_sem, vrecv_sem)):
            width = dst.shape[2]
            copy = pltpu.make_async_remote_copy(
                src_ref=src.at[0, :, pl.ds(pl.multiple_of(other * width, width), width)], dst_ref=dst.at[step],
                send_sem=ssem.at[step], recv_sem=rsem.at[step], device_id=(other,), device_id_type=MESH)
            copy.start()
            small.append(copy)

    sqa[...] = jnp.zeros_like(sqa)
    sqm[...] = jnp.zeros_like(sqm)

    def column(kind, chip_x, chip_y, owner_core, bank_length, width, chunk):
        owner = chip_y * 4 + chip_x * 2 + owner_core
        return pl.multiple_of(owner * bank_length + chunk * width, width)

    def chips(kind):
        fx, fy = x + kind * (1 - 2 * x), y + (1 - kind) * (1 - 2 * y)
        nx, ny = x + (1 - kind) * (1 - 2 * x), y + kind * (1 - 2 * y)
        return ((x, y), (fx, fy), (nx, ny), (1 - x, 1 - y))

    def first_peer(kind):
        return xn + kind * (yn - xn)

    def second_peer(kind):
        return yn + kind * (xn - yn)

    def send_one(slot, kind, bank):
        s1, r1 = banks[bank][4], banks[bank][5]
        return pltpu.make_async_remote_copy(
            src_ref=s1.at[slot], dst_ref=r1.at[slot], send_sem=send1_sem.at[bank, slot], recv_sem=recv1_sem.at[bank, slot],
            device_id=(first_peer(kind),), device_id_type=MESH)

    def send_two(slot, kind, bank):
        s2, r2 = banks[bank][6], banks[bank][7]
        return pltpu.make_async_remote_copy(
            src_ref=s2.at[slot], dst_ref=r2.at[slot], send_sem=send2_sem.at[bank, slot], recv_sem=recv2_sem.at[bank, slot],
            device_id=(second_peer(kind),), device_id_type=MESH)

    def out_copy(chunk, slot, bank):
        out, staged, width = banks[bank][1], banks[bank][8], banks[bank][10]
        return pltpu.make_async_copy(staged.at[slot], out.at[:, pl.ds(pl.multiple_of(chunk * width, width), width)], out_sem.at[bank, slot])

    def body(i, carry):
        d = i - AHEAD - LAG_TWO

        @pl.when(d >= 0)
        def _():
            slot = lax.rem(d, SLOTS)
            kind = lax.rem(d, 2)
            for bank in range(2):
                r2, staged, sq, width = banks[bank][7], banks[bank][8], banks[bank][9], banks[bank][10]
                one, two = send_one(slot, kind, bank), send_two(slot, kind, bank)
                two.wait_recv()
                one.wait_send()
                two.wait_send()
                square = sq[...]
                for at in range(0, width, 128):
                    mean = (staged[slot, :, at:at + 128] + r2[slot, :, at:at + 128]) * (1.0 / devices)
                    staged[slot, :, at:at + 128] = mean
                    square = square + mean * mean
                sq[...] = square
                out_copy(d, slot, bank).start()

            @pl.when(d + SLOTS < chunks)
            def _():
                pl.semaphore_signal(credit2.at[kind], inc=1, device_id=(second_peer(kind),), device_id_type=MESH)

        c = i - AHEAD - LAG_ONE

        @pl.when(jnp.logical_and(c >= 0, c < chunks))
        def _():
            slot = lax.rem(c, SLOTS)
            kind = lax.rem(c, 2)

            @pl.when(c >= SLOTS)
            def _():
                pl.semaphore_wait(credit2.at[kind], 1)

            for bank in range(2):
                l, p, r1, s2, staged = banks[bank][2], banks[bank][3], banks[bank][5], banks[bank][6], banks[bank][8]
                send_one(slot, kind, bank).wait_recv()
                pltpu.make_async_copy(p.at[slot], p.at[slot], psend_sem.at[bank, slot]).wait()

                @pl.when(c >= SLOTS)
                def _():
                    out_copy(c - SLOTS, slot, bank).wait()

                s2[slot] = r1[slot, 1] + (l[slot, 1].astype(jnp.float32) + p[slot, 1].astype(jnp.float32))
                send_two(slot, kind, bank).start()
                staged[slot] = r1[slot, 0] + (l[slot, 0].astype(jnp.float32) + p[slot, 0].astype(jnp.float32))

            @pl.when(c + SLOTS < chunks)
            def _():
                pl.semaphore_signal(pcredit, inc=1, device_id=(partner,), device_id_type=MESH)
                pl.semaphore_signal(credit1.at[kind], inc=1, device_id=(first_peer(kind),), device_id_type=MESH)

        b = i - AHEAD

        @pl.when(jnp.logical_and(b >= 0, b < chunks))
        def _():
            slot = lax.rem(b, SLOTS)
            kind = lax.rem(b, 2)

            @pl.when(b >= SLOTS)
            def _():
                pl.semaphore_wait(credit1.at[kind], 1)

            for bank in range(2):
                l, p, s1 = banks[bank][2], banks[bank][3], banks[bank][4]
                pltpu.make_async_copy(l.at[slot], l.at[slot], load_sem.at[bank, slot]).wait()
                pltpu.make_async_copy(p.at[slot], p.at[slot], precv_sem.at[bank, slot]).wait()
                for block in range(2):
                    s1[slot, block] = l[slot, 2 + block].astype(jnp.float32) + p[slot, 2 + block].astype(jnp.float32)
                send_one(slot, kind, bank).start()

        @pl.when(i < chunks)
        def _():
            slot = lax.rem(i, SLOTS)
            kind = lax.rem(i, 2)

            @pl.when(i >= SLOTS)
            def _():
                pl.semaphore_wait(pcredit, 1)

            for bank in range(2):
                g, l, p, width = banks[bank][0], banks[bank][2], banks[bank][3], banks[bank][10]
                length = g.shape[2] // devices
                for block, (bx, by) in enumerate(chips(kind)):
                    theirs = column(kind, bx, by, 1 - core, length, width, i)
                    pltpu.make_async_remote_copy(
                        src_ref=g.at[0, :, pl.ds(theirs, width)], dst_ref=p.at[slot, block],
                        send_sem=psend_sem.at[bank, slot], recv_sem=precv_sem.at[bank, slot],
                        device_id=(partner,), device_id_type=MESH).start()
                    mine = column(kind, bx, by, core, length, width, i)
                    pltpu.make_async_copy(g.at[0, :, pl.ds(mine, width)], l.at[slot, block], load_sem.at[bank, slot]).start()

        return carry

    lax.fori_loop(0, chunks + AHEAD + LAG_TWO, body, 0)

    for copy in small:
        copy.wait()
    square = jnp.sum(sqa[...], axis=0, keepdims=True) + jnp.sum(sqm[...], axis=0, keepdims=True)
    for src, received, out in ((gw, rw, ow), (gv, rv, ov)):
        width = received.shape[2]
        mean = src[0, :, pl.ds(pl.multiple_of(me * width, width), width)].astype(jnp.float32)
        for step in range(1, devices):
            mean = mean + received[step].astype(jnp.float32)
        mean = mean * (1.0 / devices)
        out[...] = mean
        for at in range(0, width, 128):
            part = mean[:, at:at + 128]
            square = square + jnp.sum(part * part, axis=0, keepdims=True)
    tiles[me] = jnp.broadcast_to(square, tiles.shape[1:])
    share_tile(me, devices, tiles, tsend_sem, trecv_sem)
    everything = tiles[0]
    for device in range(1, devices):
        everything = everything + tiles[device]
    total[...] = jnp.broadcast_to(jnp.sum(everything[0:1], axis=1, keepdims=True), total.shape)

    def drain(i, carry):
        chunk = chunks - SLOTS + i
        slot = lax.rem(chunk, SLOTS)
        for bank in range(2):
            out_copy(chunk, slot, bank).wait()
        return carry

    lax.fori_loop(0, SLOTS, drain, 0)


def reduce_scatter(devices, ga, gm, gw, gv):
    f32, bf16 = jnp.float32, jnp.bfloat16
    rows = (ga.shape[1], gm.shape[1])
    lengths = (ga.shape[2] // devices, gm.shape[2] // devices)
    chunks = lengths[0] // ATTN_WIDTH
    widths = (ATTN_WIDTH, lengths[1] // chunks)
    small = (gw.shape[2] // devices, gv.shape[2] // devices)

    def buffers(blocks, dtype):
        lead = (SLOTS,) if blocks == 1 else (SLOTS, blocks)
        return [pltpu.VMEM(lead + (rows[bank], widths[bank]), dtype) for bank in range(2)]

    dma = pltpu.SemaphoreType.DMA
    scratch = (
        buffers(4, bf16) + buffers(4, bf16) + buffers(2, f32) + buffers(2, f32) + buffers(1, f32) + buffers(1, f32) + buffers(1, f32)
        + [pltpu.VMEM((devices, gw.shape[1], small[0]), bf16), pltpu.VMEM((devices, gv.shape[1], small[1]), bf16)]
        + [pltpu.VMEM((rows[bank], 128), f32) for bank in range(2)] + [pltpu.VMEM((devices, 8, 128), f32)]
        + [dma((2, SLOTS))] * 8 + [dma((devices,))] * 6
        + [pltpu.SemaphoreType.REGULAR, pltpu.SemaphoreType.REGULAR((2,)), pltpu.SemaphoreType.REGULAR((2,))]
    )
    vmem = pl.BlockSpec(memory_space=pltpu.VMEM)
    anywhere = pl.BlockSpec(memory_space=pl.ANY)
    return pl.pallas_call(
        functools.partial(scatter_kernel, devices, widths, chunks),
        name="scatter",
        out_shape=[jax.ShapeDtypeStruct((rows[0], lengths[0]), f32), jax.ShapeDtypeStruct((rows[1], lengths[1]), f32),
                   jax.ShapeDtypeStruct((gw.shape[1], small[0]), f32), jax.ShapeDtypeStruct((gv.shape[1], small[1]), f32),
                   jax.ShapeDtypeStruct((8, 128), f32)],
        in_specs=[anywhere, anywhere, vmem, vmem],
        out_specs=[anywhere, anywhere, vmem, vmem, vmem],
        scratch_shapes=scratch,
        compiler_params=pltpu.CompilerParams(collective_id=0, has_side_effects=True, vmem_limit_bytes=48 * 1024 * 1024),
    )(ga, gm, gw, gv)


def share_kernel(devices, part, total, tiles, send_sem, recv_sem):
    me = lax.axis_index("data")
    signal_all_and_wait(me, devices)
    tiles[me] = part[...]
    share_tile(me, devices, tiles, send_sem, recv_sem)
    everything = tiles[0]
    for device in range(1, devices):
        everything = everything + tiles[device]
    total[...] = everything


def sum_over_devices(devices, part):
    dma = pltpu.SemaphoreType.DMA
    vmem = pl.BlockSpec(memory_space=pltpu.VMEM)
    return pl.pallas_call(
        functools.partial(share_kernel, devices),
        name="share",
        out_shape=jax.ShapeDtypeStruct(part.shape, part.dtype),
        in_specs=[vmem],
        out_specs=vmem,
        scratch_shapes=[pltpu.VMEM((devices,) + part.shape, part.dtype), dma((devices,)), dma((devices,))],
        compiler_params=pltpu.CompilerParams(collective_id=1, has_side_effects=True),
    )(part)


def adam_direction(mean_grad, weight, first_moment, second_moment, clip_coef):
    clipped = clip_coef * mean_grad
    new_first = BETA_FIRST * first_moment + (1.0 - BETA_FIRST) * clipped
    new_second = BETA_SECOND * second_moment + (1.0 - BETA_SECOND) * (clipped * clipped)
    update = (new_first / (1.0 - BETA_FIRST ** STEP_NUMBER)) / (jnp.sqrt(new_second / (1.0 - BETA_SECOND ** STEP_NUMBER)) + EPSILON) + WEIGHT_DECAY * weight
    return update, new_first, new_second


def solution(mesh):
    group_size = mesh.shape["data"]
    grad_spec = P("data", None, None)
    shard_spec = P(None, "data")
    full_spec = P(None, None)

    def local_step(*all_banks):
        weights = all_banks[4:8]
        firsts = all_banks[8:12]
        seconds = all_banks[12:16]
        *mean_grads, total_square = reduce_scatter(group_size, *all_banks[0:4])
        clip_coef = jnp.minimum(1.0, MAX_NORM / jnp.sqrt(total_square[0, 0]))
        results = [adam_direction(mean_grads[bank_index], weights[bank_index], firsts[bank_index], seconds[bank_index], clip_coef) for bank_index in range(4)]
        part_sums = jnp.concatenate([jnp.sum(weight * weight, axis=1) for weight in weights] + [jnp.sum(result[0] * result[0], axis=1) for result in results])
        count = part_sums.shape[0]
        tile = jnp.pad(part_sums, (0, 1024 - count)).reshape(8, 128)
        norm_sums = sum_over_devices(group_size, tile).reshape(1024)[:count]
        tensor_count = norm_sums.shape[0] // 2
        trust_ratios = jnp.sqrt(norm_sums[:tensor_count]) / jnp.sqrt(norm_sums[tensor_count:])
        replicas, new_weights = [], []
        first_row = 0
        for bank_index in range(4):
            row_count = weights[bank_index].shape[0]
            trust_ratio = trust_ratios[first_row:first_row + row_count]
            first_row = first_row + row_count
            new_weight = weights[bank_index] - LEARN_RATE * trust_ratio[:, None] * results[bank_index][0]
            new_weights.append(new_weight)
            replicas.append(lax.all_gather(new_weight.astype(jnp.bfloat16), "data", axis=1, tiled=True))
        return tuple(replicas + new_weights + [result[1] for result in results] + [result[2] for result in results])

    return jax.shard_map(local_step, mesh=mesh, in_specs=(grad_spec,) * 4 + (shard_spec,) * 12, out_specs=(full_spec,) * 4 + (shard_spec,) * 12, check_vma=False)
```

```python
import functools

import jax
import jax.numpy as jnp
from jax import lax
from jax.experimental import pallas as pl
from jax.experimental.pallas import tpu as pltpu
from jax.sharding import PartitionSpec as P

STEP_NUMBER = 10
LEARN_RATE = 0.04
BETA_FIRST = 0.9
BETA_SECOND = 0.999
EPSILON = 1e-6
WEIGHT_DECAY = 0.01
MAX_NORM = 1.0

MESH = pl.DeviceIdType.MESH
SLOTS = 8
AHEAD = 2
LAG_ONE = 4
LAG_TWO = 8
WIDTH = 1024
OUT_SLOTS = 4


def signal_all_and_wait(me, devices):
    barrier = pltpu.get_barrier_semaphore()
    for step in range(1, devices):
        pl.semaphore_signal(barrier, inc=1, device_id=(lax.rem(me + step, devices),), device_id_type=MESH)
    pl.semaphore_wait(barrier, devices - 1)


def share_tile(me, devices, tiles, send_sem, recv_sem):
    copies = []
    for step in range(1, devices):
        other = lax.rem(me + step, devices)
        copy = pltpu.make_async_remote_copy(
            src_ref=tiles.at[me], dst_ref=tiles.at[me], send_sem=send_sem.at[step], recv_sem=recv_sem.at[step],
            device_id=(other,), device_id_type=MESH)
        copy.start()
        copies.append(copy)
    for copy in copies:
        copy.wait()


def pieces(width):
    half, wide = width // 2, 4 * width
    first = width + half
    return (
        (0, (0, 8), (0, width), (0, 8), (0, width)),
        (0, (8, 12), (0, half), (0, 4), (width, first)),
        (0, (8, 12), (half, width), (4, 8), (width, first)),
        (1, (0, 6), (0, 3 * width), (0, 6), (first, first + 3 * width)),
        (1, (0, 2), (3 * width, wide), (6, 8), (first, first + width)),
        (1, (2, 4), (3 * width, wide), (6, 8), (first + width, first + 2 * width)),
        (1, (4, 6), (3 * width, wide), (6, 8), (first + 2 * width, first + 3 * width)),
    )


def scatter_kernel(devices, width, chunks, ga, gm, gw, gv, oa, om, ow, ov, total,
                   la, lm, pa, pm, s1, r1, s2, r2, staged, ua, um, rw, rv, sq, tiles,
                   load_sem, psend_sem, precv_sem, out_sem, send1_sem, recv1_sem, send2_sem, recv2_sem,
                   wsend_sem, wrecv_sem, vsend_sem, vrecv_sem, tsend_sem, trecv_sem, pcredit, credit1, credit2):
    me = lax.axis_index("data")
    core = lax.rem(me, 2)
    x = lax.rem(me // 2, 2)
    y = me // 4
    partner = me + 1 - 2 * core
    xn = y * 4 + (1 - x) * 2 + core
    yn = (1 - y) * 4 + x * 2 + core
    banks = ((ga, oa, la, pa, ua, width), (gm, om, lm, pm, um, 4 * width))

    signal_all_and_wait(me, devices)

    small = []
    for step in range(1, devices):
        other = lax.rem(me + step, devices)
        for src, dst, ssem, rsem in ((gw, rw, wsend_sem, wrecv_sem), (gv, rv, vsend_sem, vrecv_sem)):
            small_width = dst.shape[2]
            copy = pltpu.make_async_remote_copy(
                src_ref=src.at[0, :, pl.ds(pl.multiple_of(other * small_width, small_width), small_width)], dst_ref=dst.at[step],
                send_sem=ssem.at[step], recv_sem=rsem.at[step], device_id=(other,), device_id_type=MESH)
            copy.start()
            small.append(copy)

    sq[...] = jnp.zeros_like(sq)

    def chips(kind):
        fx, fy = x + kind * (1 - 2 * x), y + (1 - kind) * (1 - 2 * y)
        nx, ny = x + (1 - kind) * (1 - 2 * x), y + kind * (1 - 2 * y)
        return ((x, y), (fx, fy), (nx, ny), (1 - x, 1 - y))

    def first_peer(kind):
        return xn + kind * (yn - xn)

    def second_peer(kind):
        return yn + kind * (xn - yn)

    def send_one(slot, kind):
        return pltpu.make_async_remote_copy(
            src_ref=s1.at[slot], dst_ref=r1.at[slot], send_sem=send1_sem.at[slot], recv_sem=recv1_sem.at[slot],
            device_id=(first_peer(kind),), device_id_type=MESH)

    def send_two(slot, kind):
        return pltpu.make_async_remote_copy(
            src_ref=s2.at[slot], dst_ref=r2.at[slot], send_sem=send2_sem.at[slot], recv_sem=recv2_sem.at[slot],
            device_id=(second_peer(kind),), device_id_type=MESH)

    def out_copy(chunk, bank):
        out, unpacked, columns = banks[bank][1], banks[bank][4], banks[bank][5]
        slot = lax.rem(chunk, OUT_SLOTS)
        return pltpu.make_async_copy(unpacked.at[slot], out.at[:, pl.ds(pl.multiple_of(chunk * columns, columns), columns)], out_sem.at[bank, slot])

    def pair_sums(slot, block):
        return [banks[bank][2][slot, block].astype(jnp.float32) + banks[bank][3][slot, block].astype(jnp.float32) for bank in range(2)]

    def body(i, carry):
        d = i - AHEAD - LAG_TWO

        @pl.when(d >= 0)
        def _():
            slot = lax.rem(d, SLOTS)
            kind = lax.rem(d, 2)
            send_two(slot, kind).wait_recv()

            @pl.when(d >= OUT_SLOTS)
            def _():
                for bank in range(2):
                    out_copy(d - OUT_SLOTS, bank).wait()

            square = sq[...]
            for at in range(0, s2.shape[2], 128):
                mean = (staged[slot, :, at:at + 128] + r2[slot, :, at:at + 128]) * (1.0 / devices)
                staged[slot, :, at:at + 128] = mean
                square = square + mean * mean
            sq[...] = square
            out_slot = lax.rem(d, OUT_SLOTS)
            for bank, rows, columns, packed_rows, packed_columns in pieces(width):
                banks[bank][4][out_slot, rows[0]:rows[1], columns[0]:columns[1]] = staged[slot, packed_rows[0]:packed_rows[1], packed_columns[0]:packed_columns[1]]
            for bank in range(2):
                out_copy(d, bank).start()

            @pl.when(d + SLOTS < chunks)
            def _():
                pl.semaphore_signal(credit2.at[kind], inc=1, device_id=(second_peer(kind),), device_id_type=MESH)

            send_one(slot, kind).wait_send()
            send_two(slot, kind).wait_send()

        c = i - AHEAD - LAG_ONE

        @pl.when(jnp.logical_and(c >= 0, c < chunks))
        def _():
            slot = lax.rem(c, SLOTS)
            kind = lax.rem(c, 2)

            @pl.when(c >= SLOTS)
            def _():
                pl.semaphore_wait(credit2.at[kind], 1)

            send_one(slot, kind).wait_recv()
            sums = pair_sums(slot, 1)
            for bank, rows, columns, packed_rows, packed_columns in pieces(width):
                at = (slice(*packed_rows), slice(*packed_columns))
                s2[(slot, *at)] = r1[(slot, 1, *at)] + sums[bank][rows[0]:rows[1], columns[0]:columns[1]]
            send_two(slot, kind).start()
            sums = pair_sums(slot, 0)
            for bank, rows, columns, packed_rows, packed_columns in pieces(width):
                at = (slice(*packed_rows), slice(*packed_columns))
                staged[(slot, *at)] = r1[(slot, 0, *at)] + sums[bank][rows[0]:rows[1], columns[0]:columns[1]]

            @pl.when(c + SLOTS < chunks)
            def _():
                pl.semaphore_signal(pcredit, inc=1, device_id=(partner,), device_id_type=MESH)
                pl.semaphore_signal(credit1.at[kind], inc=1, device_id=(first_peer(kind),), device_id_type=MESH)

            for bank in range(2):
                p = banks[bank][3]
                pltpu.make_async_copy(p.at[slot], p.at[slot], psend_sem.at[bank, slot]).wait()

        b = i - AHEAD

        @pl.when(jnp.logical_and(b >= 0, b < chunks))
        def _():
            slot = lax.rem(b, SLOTS)
            kind = lax.rem(b, 2)

            @pl.when(b >= SLOTS)
            def _():
                pl.semaphore_wait(credit1.at[kind], 1)

            for bank in range(2):
                l, p = banks[bank][2], banks[bank][3]
                pltpu.make_async_copy(l.at[slot], l.at[slot], load_sem.at[bank, slot]).wait()
                pltpu.make_async_copy(p.at[slot], p.at[slot], precv_sem.at[bank, slot]).wait()
            for block in range(2):
                sums = pair_sums(slot, 2 + block)
                for bank, rows, columns, packed_rows, packed_columns in pieces(width):
                    s1[slot, block, packed_rows[0]:packed_rows[1], packed_columns[0]:packed_columns[1]] = sums[bank][rows[0]:rows[1], columns[0]:columns[1]]
            send_one(slot, kind).start()

        @pl.when(i < chunks)
        def _():
            slot = lax.rem(i, SLOTS)
            kind = lax.rem(i, 2)

            @pl.when(i >= SLOTS)
            def _():
                pl.semaphore_wait(pcredit, 1)

            for bank in range(2):
                g, l, p, columns = banks[bank][0], banks[bank][2], banks[bank][3], banks[bank][5]
                length = g.shape[2] // devices
                for block, (bx, by) in enumerate(chips(kind)):
                    chip = by * 4 + bx * 2
                    theirs = pl.multiple_of((chip + 1 - core) * length + i * columns, columns)
                    pltpu.make_async_remote_copy(
                        src_ref=g.at[0, :, pl.ds(theirs, columns)], dst_ref=p.at[slot, block],
                        send_sem=psend_sem.at[bank, slot], recv_sem=precv_sem.at[bank, slot],
                        device_id=(partner,), device_id_type=MESH).start()
                    mine = pl.multiple_of((chip + core) * length + i * columns, columns)
                    pltpu.make_async_copy(g.at[0, :, pl.ds(mine, columns)], l.at[slot, block], load_sem.at[bank, slot]).start()

        return carry

    lax.fori_loop(0, chunks + AHEAD + LAG_TWO, body, 0)

    for copy in small:
        copy.wait()
    square = jnp.sum(sq[...], axis=0, keepdims=True)
    for src, received, out in ((gw, rw, ow), (gv, rv, ov)):
        small_width = received.shape[2]
        mean = src[0, :, pl.ds(pl.multiple_of(me * small_width, small_width), small_width)].astype(jnp.float32)
        for step in range(1, devices):
            mean = mean + received[step].astype(jnp.float32)
        mean = mean * (1.0 / devices)
        out[...] = mean
        for at in range(0, small_width, 128):
            part = mean[:, at:at + 128]
            square = square + jnp.sum(part * part, axis=0, keepdims=True)
    tiles[me] = jnp.broadcast_to(square, tiles.shape[1:])
    share_tile(me, devices, tiles, tsend_sem, trecv_sem)
    everything = tiles[0]
    for device in range(1, devices):
        everything = everything + tiles[device]
    total[...] = jnp.broadcast_to(jnp.sum(everything[0:1], axis=1, keepdims=True), total.shape)

    for chunk in range(chunks - OUT_SLOTS, chunks):
        for bank in range(2):
            out_copy(chunk, bank).wait()


def reduce_scatter(devices, ga, gm, gw, gv):
    f32, bf16 = jnp.float32, jnp.bfloat16
    rows = (ga.shape[1], gm.shape[1])
    lengths = (ga.shape[2] // devices, gm.shape[2] // devices)
    chunks = lengths[0] // WIDTH
    widths = (WIDTH, lengths[1] // chunks)
    small = (gw.shape[2] // devices, gv.shape[2] // devices)
    packed = (rows[0] * widths[0] + rows[1] * widths[1]) // 8

    def unpacked(lead, dtype):
        return [pltpu.VMEM(lead + (rows[bank], widths[bank]), dtype) for bank in range(2)]

    dma = pltpu.SemaphoreType.DMA
    scratch = (
        unpacked((SLOTS, 4), bf16) + unpacked((SLOTS, 4), bf16)
        + [pltpu.VMEM((SLOTS, 2, 8, packed), f32)] * 2 + [pltpu.VMEM((SLOTS, 8, packed), f32)] * 3
        + unpacked((OUT_SLOTS,), f32)
        + [pltpu.VMEM((devices, gw.shape[1], small[0]), bf16), pltpu.VMEM((devices, gv.shape[1], small[1]), bf16)]
        + [pltpu.VMEM((8, 128), f32), pltpu.VMEM((devices, 8, 128), f32)]
        + [dma((2, SLOTS))] * 3 + [dma((2, OUT_SLOTS))] + [dma((SLOTS,))] * 4 + [dma((devices,))] * 6
        + [pltpu.SemaphoreType.REGULAR, pltpu.SemaphoreType.REGULAR((2,)), pltpu.SemaphoreType.REGULAR((2,))]
    )
    vmem = pl.BlockSpec(memory_space=pltpu.VMEM)
    anywhere = pl.BlockSpec(memory_space=pl.ANY)
    return pl.pallas_call(
        functools.partial(scatter_kernel, devices, WIDTH, chunks),
        name="scatter",
        out_shape=[jax.ShapeDtypeStruct((rows[0], lengths[0]), f32), jax.ShapeDtypeStruct((rows[1], lengths[1]), f32),
                   jax.ShapeDtypeStruct((gw.shape[1], small[0]), f32), jax.ShapeDtypeStruct((gv.shape[1], small[1]), f32),
                   jax.ShapeDtypeStruct((8, 128), f32)],
        in_specs=[anywhere, anywhere, vmem, vmem],
        out_specs=[anywhere, anywhere, vmem, vmem, vmem],
        scratch_shapes=scratch,
        compiler_params=pltpu.CompilerParams(collective_id=0, has_side_effects=True, vmem_limit_bytes=48 * 1024 * 1024),
    )(ga, gm, gw, gv)


def share_kernel(devices, part, total, tiles, send_sem, recv_sem):
    me = lax.axis_index("data")
    signal_all_and_wait(me, devices)
    tiles[me] = part[...]
    share_tile(me, devices, tiles, send_sem, recv_sem)
    everything = tiles[0]
    for device in range(1, devices):
        everything = everything + tiles[device]
    total[...] = everything


def sum_over_devices(devices, part):
    dma = pltpu.SemaphoreType.DMA
    vmem = pl.BlockSpec(memory_space=pltpu.VMEM)
    return pl.pallas_call(
        functools.partial(share_kernel, devices),
        name="share",
        out_shape=jax.ShapeDtypeStruct(part.shape, part.dtype),
        in_specs=[vmem],
        out_specs=vmem,
        scratch_shapes=[pltpu.VMEM((devices,) + part.shape, part.dtype), dma((devices,)), dma((devices,))],
        compiler_params=pltpu.CompilerParams(collective_id=1, has_side_effects=True),
    )(part)


def adam_direction(mean_grad, weight, first_moment, second_moment, clip_coef):
    clipped = clip_coef * mean_grad
    new_first = BETA_FIRST * first_moment + (1.0 - BETA_FIRST) * clipped
    new_second = BETA_SECOND * second_moment + (1.0 - BETA_SECOND) * (clipped * clipped)
    update = (new_first / (1.0 - BETA_FIRST ** STEP_NUMBER)) / (jnp.sqrt(new_second / (1.0 - BETA_SECOND ** STEP_NUMBER)) + EPSILON) + WEIGHT_DECAY * weight
    return update, new_first, new_second


def solution(mesh):
    group_size = mesh.shape["data"]
    grad_spec = P("data", None, None)
    shard_spec = P(None, "data")
    full_spec = P(None, None)

    def local_step(*all_banks):
        weights = all_banks[4:8]
        firsts = all_banks[8:12]
        seconds = all_banks[12:16]
        *mean_grads, total_square = reduce_scatter(group_size, *all_banks[0:4])
        clip_coef = jnp.minimum(1.0, MAX_NORM / jnp.sqrt(total_square[0, 0]))
        results = [adam_direction(mean_grads[bank_index], weights[bank_index], firsts[bank_index], seconds[bank_index], clip_coef) for bank_index in range(4)]
        part_sums = jnp.concatenate([jnp.sum(weight * weight, axis=1) for weight in weights] + [jnp.sum(result[0] * result[0], axis=1) for result in results])
        count = part_sums.shape[0]
        tile = jnp.pad(part_sums, (0, 1024 - count)).reshape(8, 128)
        norm_sums = sum_over_devices(group_size, tile).reshape(1024)[:count]
        tensor_count = norm_sums.shape[0] // 2
        trust_ratios = jnp.sqrt(norm_sums[:tensor_count]) / jnp.sqrt(norm_sums[tensor_count:])
        replicas, new_weights = [], []
        first_row = 0
        for bank_index in range(4):
            row_count = weights[bank_index].shape[0]
            trust_ratio = trust_ratios[first_row:first_row + row_count]
            first_row = first_row + row_count
            new_weight = weights[bank_index] - LEARN_RATE * trust_ratio[:, None] * results[bank_index][0]
            new_weights.append(new_weight)
            replicas.append(lax.all_gather(new_weight.astype(jnp.bfloat16), "data", axis=1, tiled=True))
        return tuple(replicas + new_weights + [result[1] for result in results] + [result[2] for result in results])

    return jax.shard_map(local_step, mesh=mesh, in_specs=(grad_spec,) * 4 + (shard_spec,) * 12, out_specs=(full_spec,) * 4 + (shard_spec,) * 12, check_vma=False)
```

```python
import functools

import jax
import jax.numpy as jnp
from jax import lax
from jax.experimental import pallas as pl
from jax.experimental.pallas import tpu as pltpu
from jax.sharding import PartitionSpec as P

STEP_NUMBER = 10
LEARN_RATE = 0.04
BETA_FIRST = 0.9
BETA_SECOND = 0.999
EPSILON = 1e-6
WEIGHT_DECAY = 0.01
MAX_NORM = 1.0

MESH = pl.DeviceIdType.MESH
SLOTS = 8
AHEAD = 2
LAG_ONE = 4
LAG_TWO = 8
WIDTH = 1024
OUT_SLOTS = 4
ATTN_BLOCK = 8192
MLP_BLOCK = 16384
MLP_SPLITS = (12, 10, 6, 4)


def signal_all_and_wait(me, devices):
    barrier = pltpu.get_barrier_semaphore()
    for step in range(1, devices):
        pl.semaphore_signal(barrier, inc=1, device_id=(lax.rem(me + step, devices),), device_id_type=MESH)
    pl.semaphore_wait(barrier, devices - 1)


def share_tile(me, devices, tiles, send_sem, recv_sem):
    copies = []
    for step in range(1, devices):
        other = lax.rem(me + step, devices)
        copy = pltpu.make_async_remote_copy(
            src_ref=tiles.at[me], dst_ref=tiles.at[me], send_sem=send_sem.at[step], recv_sem=recv_sem.at[step],
            device_id=(other,), device_id_type=MESH)
        copy.start()
        copies.append(copy)
    for copy in copies:
        copy.wait()


def pieces(width):
    half, wide = width // 2, 4 * width
    first = width + half
    return (
        (0, (0, 8), (0, width), (0, 8), (0, width)),
        (0, (8, 12), (0, half), (0, 4), (width, first)),
        (0, (8, 12), (half, width), (4, 8), (width, first)),
        (1, (0, 6), (0, 3 * width), (0, 6), (first, first + 3 * width)),
        (1, (0, 2), (3 * width, wide), (6, 8), (first, first + width)),
        (1, (2, 4), (3 * width, wide), (6, 8), (first + width, first + 2 * width)),
        (1, (4, 6), (3 * width, wide), (6, 8), (first + 2 * width, first + 3 * width)),
    )


def scatter_kernel(devices, width, chunks, ga, gm, gw, gv, oa, om, ow, ov, total,
                   la, lm, pa, pm, s1, r1, s2, r2, staged, ua, um, rw, rv, sq, tiles,
                   load_sem, psend_sem, precv_sem, out_sem, send1_sem, recv1_sem, send2_sem, recv2_sem,
                   wsend_sem, wrecv_sem, vsend_sem, vrecv_sem, tsend_sem, trecv_sem, pcredit, credit1, credit2):
    me = lax.axis_index("data")
    core = lax.rem(me, 2)
    x = lax.rem(me // 2, 2)
    y = me // 4
    partner = me + 1 - 2 * core
    xn = y * 4 + (1 - x) * 2 + core
    yn = (1 - y) * 4 + x * 2 + core
    banks = ((ga, oa, la, pa, ua, width), (gm, om, lm, pm, um, 4 * width))

    signal_all_and_wait(me, devices)

    small = []
    for step in range(1, devices):
        other = lax.rem(me + step, devices)
        for src, dst, ssem, rsem in ((gw, rw, wsend_sem, wrecv_sem), (gv, rv, vsend_sem, vrecv_sem)):
            small_width = dst.shape[2]
            copy = pltpu.make_async_remote_copy(
                src_ref=src.at[0, :, pl.ds(pl.multiple_of(other * small_width, small_width), small_width)], dst_ref=dst.at[step],
                send_sem=ssem.at[step], recv_sem=rsem.at[step], device_id=(other,), device_id_type=MESH)
            copy.start()
            small.append(copy)

    sq[...] = jnp.zeros_like(sq)

    def chips(kind):
        fx, fy = x + kind * (1 - 2 * x), y + (1 - kind) * (1 - 2 * y)
        nx, ny = x + (1 - kind) * (1 - 2 * x), y + kind * (1 - 2 * y)
        return ((x, y), (fx, fy), (nx, ny), (1 - x, 1 - y))

    def first_peer(kind):
        return xn + kind * (yn - xn)

    def second_peer(kind):
        return yn + kind * (xn - yn)

    def send_one(slot, kind):
        return pltpu.make_async_remote_copy(
            src_ref=s1.at[slot], dst_ref=r1.at[slot], send_sem=send1_sem.at[slot], recv_sem=recv1_sem.at[slot],
            device_id=(first_peer(kind),), device_id_type=MESH)

    def send_two(slot, kind):
        return pltpu.make_async_remote_copy(
            src_ref=s2.at[slot], dst_ref=r2.at[slot], send_sem=send2_sem.at[slot], recv_sem=recv2_sem.at[slot],
            device_id=(second_peer(kind),), device_id_type=MESH)

    def out_copy(chunk, bank):
        out, unpacked, columns = banks[bank][1], banks[bank][4], banks[bank][5]
        slot = lax.rem(chunk, OUT_SLOTS)
        return pltpu.make_async_copy(unpacked.at[slot], out.at[:, pl.ds(pl.multiple_of(chunk * columns, columns), columns)], out_sem.at[bank, slot])

    def pair_sums(slot, block):
        return [banks[bank][2][slot, block].astype(jnp.float32) + banks[bank][3][slot, block].astype(jnp.float32) for bank in range(2)]

    def body(i, carry):
        d = i - AHEAD - LAG_TWO

        @pl.when(d >= 0)
        def _():
            slot = lax.rem(d, SLOTS)
            kind = lax.rem(d, 2)
            send_two(slot, kind).wait_recv()

            @pl.when(d >= OUT_SLOTS)
            def _():
                for bank in range(2):
                    out_copy(d - OUT_SLOTS, bank).wait()

            square = sq[...]
            for at in range(0, s2.shape[2], 128):
                mean = (staged[slot, :, at:at + 128] + r2[slot, :, at:at + 128]) * (1.0 / devices)
                staged[slot, :, at:at + 128] = mean
                square = square + mean * mean
            sq[...] = square
            out_slot = lax.rem(d, OUT_SLOTS)
            for bank, rows, columns, packed_rows, packed_columns in pieces(width):
                banks[bank][4][out_slot, rows[0]:rows[1], columns[0]:columns[1]] = staged[slot, packed_rows[0]:packed_rows[1], packed_columns[0]:packed_columns[1]]
            for bank in range(2):
                out_copy(d, bank).start()

            @pl.when(d + SLOTS < chunks)
            def _():
                pl.semaphore_signal(credit2.at[kind], inc=1, device_id=(second_peer(kind),), device_id_type=MESH)

            send_one(slot, kind).wait_send()
            send_two(slot, kind).wait_send()

        c = i - AHEAD - LAG_ONE

        @pl.when(jnp.logical_and(c >= 0, c < chunks))
        def _():
            slot = lax.rem(c, SLOTS)
            kind = lax.rem(c, 2)

            @pl.when(c >= SLOTS)
            def _():
                pl.semaphore_wait(credit2.at[kind], 1)

            send_one(slot, kind).wait_recv()
            sums = pair_sums(slot, 1)
            for bank, rows, columns, packed_rows, packed_columns in pieces(width):
                at = (slice(*packed_rows), slice(*packed_columns))
                s2[(slot, *at)] = r1[(slot, 1, *at)] + sums[bank][rows[0]:rows[1], columns[0]:columns[1]]
            send_two(slot, kind).start()
            sums = pair_sums(slot, 0)
            for bank, rows, columns, packed_rows, packed_columns in pieces(width):
                at = (slice(*packed_rows), slice(*packed_columns))
                staged[(slot, *at)] = r1[(slot, 0, *at)] + sums[bank][rows[0]:rows[1], columns[0]:columns[1]]

            @pl.when(c + SLOTS < chunks)
            def _():
                pl.semaphore_signal(pcredit, inc=1, device_id=(partner,), device_id_type=MESH)
                pl.semaphore_signal(credit1.at[kind], inc=1, device_id=(first_peer(kind),), device_id_type=MESH)

            for bank in range(2):
                p = banks[bank][3]
                pltpu.make_async_copy(p.at[slot], p.at[slot], psend_sem.at[bank, slot]).wait()

        b = i - AHEAD

        @pl.when(jnp.logical_and(b >= 0, b < chunks))
        def _():
            slot = lax.rem(b, SLOTS)
            kind = lax.rem(b, 2)

            @pl.when(b >= SLOTS)
            def _():
                pl.semaphore_wait(credit1.at[kind], 1)

            for bank in range(2):
                l, p = banks[bank][2], banks[bank][3]
                pltpu.make_async_copy(l.at[slot], l.at[slot], load_sem.at[bank, slot]).wait()
                pltpu.make_async_copy(p.at[slot], p.at[slot], precv_sem.at[bank, slot]).wait()
            for block in range(2):
                sums = pair_sums(slot, 2 + block)
                for bank, rows, columns, packed_rows, packed_columns in pieces(width):
                    s1[slot, block, packed_rows[0]:packed_rows[1], packed_columns[0]:packed_columns[1]] = sums[bank][rows[0]:rows[1], columns[0]:columns[1]]
            send_one(slot, kind).start()

        @pl.when(i < chunks)
        def _():
            slot = lax.rem(i, SLOTS)
            kind = lax.rem(i, 2)

            @pl.when(i >= SLOTS)
            def _():
                pl.semaphore_wait(pcredit, 1)

            for bank in range(2):
                g, l, p, columns = banks[bank][0], banks[bank][2], banks[bank][3], banks[bank][5]
                length = g.shape[2] // devices
                for block, (bx, by) in enumerate(chips(kind)):
                    chip = by * 4 + bx * 2
                    theirs = pl.multiple_of((chip + 1 - core) * length + i * columns, columns)
                    pltpu.make_async_remote_copy(
                        src_ref=g.at[0, :, pl.ds(theirs, columns)], dst_ref=p.at[slot, block],
                        send_sem=psend_sem.at[bank, slot], recv_sem=precv_sem.at[bank, slot],
                        device_id=(partner,), device_id_type=MESH).start()
                    mine = pl.multiple_of((chip + core) * length + i * columns, columns)
                    pltpu.make_async_copy(g.at[0, :, pl.ds(mine, columns)], l.at[slot, block], load_sem.at[bank, slot]).start()

        return carry

    lax.fori_loop(0, chunks + AHEAD + LAG_TWO, body, 0)

    for copy in small:
        copy.wait()
    square = jnp.sum(sq[...], axis=0, keepdims=True)
    for src, received, out in ((gw, rw, ow), (gv, rv, ov)):
        small_width = received.shape[2]
        mean = src[0, :, pl.ds(pl.multiple_of(me * small_width, small_width), small_width)].astype(jnp.float32)
        for step in range(1, devices):
            mean = mean + received[step].astype(jnp.float32)
        mean = mean * (1.0 / devices)
        out[...] = mean
        for at in range(0, small_width, 128):
            part = mean[:, at:at + 128]
            square = square + jnp.sum(part * part, axis=0, keepdims=True)
    tiles[me] = jnp.broadcast_to(square, tiles.shape[1:])
    share_tile(me, devices, tiles, tsend_sem, trecv_sem)
    everything = tiles[0]
    for device in range(1, devices):
        everything = everything + tiles[device]
    total[...] = jnp.broadcast_to(jnp.sum(everything[0:1], axis=1, keepdims=True), total.shape)

    for chunk in range(chunks - OUT_SLOTS, chunks):
        for bank in range(2):
            out_copy(chunk, bank).wait()


def reduce_scatter(devices, ga, gm, gw, gv):
    f32, bf16 = jnp.float32, jnp.bfloat16
    rows = (ga.shape[1], gm.shape[1])
    lengths = (ga.shape[2] // devices, gm.shape[2] // devices)
    chunks = lengths[0] // WIDTH
    widths = (WIDTH, lengths[1] // chunks)
    small = (gw.shape[2] // devices, gv.shape[2] // devices)
    packed = (rows[0] * widths[0] + rows[1] * widths[1]) // 8

    def unpacked(lead, dtype):
        return [pltpu.VMEM(lead + (rows[bank], widths[bank]), dtype) for bank in range(2)]

    dma = pltpu.SemaphoreType.DMA
    scratch = (
        unpacked((SLOTS, 4), bf16) + unpacked((SLOTS, 4), bf16)
        + [pltpu.VMEM((SLOTS, 2, 8, packed), f32)] * 2 + [pltpu.VMEM((SLOTS, 8, packed), f32)] * 3
        + unpacked((OUT_SLOTS,), f32)
        + [pltpu.VMEM((devices, gw.shape[1], small[0]), bf16), pltpu.VMEM((devices, gv.shape[1], small[1]), bf16)]
        + [pltpu.VMEM((8, 128), f32), pltpu.VMEM((devices, 8, 128), f32)]
        + [dma((2, SLOTS))] * 3 + [dma((2, OUT_SLOTS))] + [dma((SLOTS,))] * 4 + [dma((devices,))] * 6
        + [pltpu.SemaphoreType.REGULAR, pltpu.SemaphoreType.REGULAR((2,)), pltpu.SemaphoreType.REGULAR((2,))]
    )
    vmem = pl.BlockSpec(memory_space=pltpu.VMEM)
    anywhere = pl.BlockSpec(memory_space=pl.ANY)
    return pl.pallas_call(
        functools.partial(scatter_kernel, devices, WIDTH, chunks),
        name="scatter",
        out_shape=[jax.ShapeDtypeStruct((rows[0], lengths[0]), f32), jax.ShapeDtypeStruct((rows[1], lengths[1]), f32),
                   jax.ShapeDtypeStruct((gw.shape[1], small[0]), f32), jax.ShapeDtypeStruct((gv.shape[1], small[1]), f32),
                   jax.ShapeDtypeStruct((8, 128), f32)],
        in_specs=[anywhere, anywhere, vmem, vmem],
        out_specs=[anywhere, anywhere, vmem, vmem, vmem],
        scratch_shapes=scratch,
        compiler_params=pltpu.CompilerParams(collective_id=0, has_side_effects=True, vmem_limit_bytes=48 * 1024 * 1024),
    )(ga, gm, gw, gv)


def adam_direction(mean_grad, weight, first_moment, second_moment, clip_coef):
    clipped = clip_coef * mean_grad
    new_first = BETA_FIRST * first_moment + (1.0 - BETA_FIRST) * clipped
    new_second = BETA_SECOND * second_moment + (1.0 - BETA_SECOND) * (clipped * clipped)
    update = (new_first / (1.0 - BETA_FIRST ** STEP_NUMBER)) / (jnp.sqrt(new_second / (1.0 - BETA_SECOND ** STEP_NUMBER)) + EPSILON) + WEIGHT_DECAY * weight
    return update, new_first, new_second


def share_kernel(devices, part, total, tiles, send_sem, recv_sem):
    me = lax.axis_index("data")
    signal_all_and_wait(me, devices)
    tiles[me] = part[...]
    share_tile(me, devices, tiles, send_sem, recv_sem)
    everything = tiles[0]
    for device in range(1, devices):
        everything = everything + tiles[device]
    if total.shape == part.shape:
        total[...] = everything
    else:
        weight_norm = jnp.sqrt(jnp.sum(everything[0:8], axis=1, keepdims=True))
        update_norm = jnp.sqrt(jnp.sum(everything[8:16], axis=1, keepdims=True))
        total[...] = jnp.broadcast_to(LEARN_RATE * (weight_norm / update_norm), total.shape)


def sum_over_devices(devices, part, name, collective_id, ratio):
    dma = pltpu.SemaphoreType.DMA
    vmem = pl.BlockSpec(memory_space=pltpu.VMEM)
    return pl.pallas_call(
        functools.partial(share_kernel, devices),
        name=name,
        out_shape=jax.ShapeDtypeStruct((8, 128) if ratio else part.shape, part.dtype),
        in_specs=[vmem],
        out_specs=vmem,
        scratch_shapes=[pltpu.VMEM((devices,) + part.shape, part.dtype), dma((devices,)), dma((devices,))],
        compiler_params=pltpu.CompilerParams(collective_id=collective_id, has_side_effects=True),
    )(part)


def moment_kernel(valid, g, w, m, v, total, *refs):
    new_m, new_v, u, norms = refs[-4:]
    clip = jnp.minimum(1.0, MAX_NORM / jnp.sqrt(total[...]))

    @pl.when(pl.program_id(0) == 0)
    def _():
        norms[...] = jnp.zeros_like(norms)

    def step(index, carry):
        weight_square, update_square = carry
        for part in range(8):
            at = pl.ds(pl.multiple_of(index * 1024 + part * 128, 128), 128)
            weight = w[:, at]
            update, first, second = adam_direction(g[:, at], weight, m[:, at], v[:, at], clip)
            new_m[:, at] = first
            new_v[:, at] = second
            u[:, at] = update
            weight_square = weight_square + weight * weight
            update_square = update_square + update * update
        return weight_square, update_square

    zero = jnp.zeros((8, 128), jnp.float32)
    weight_square, update_square = lax.fori_loop(0, g.shape[1] // 1024, step, (zero, zero))
    row = lax.broadcasted_iota(jnp.int32, (8, 128), 0)
    norms[0:8] += jnp.where(row < valid, weight_square, 0.0)
    norms[8:16] += jnp.where(row < valid, update_square, 0.0)


def moments(name, row_block, valid, block, g, w, m, v, total, before=()):
    f32 = jnp.float32
    rows, length = g.shape
    columns = pl.BlockSpec((8, block), lambda i: (row_block, i))
    whole = jax.ShapeDtypeStruct((rows, length), f32)
    bytes_moved = 8 * length * 4 * 7
    return pl.pallas_call(
        functools.partial(moment_kernel, valid),
        name=name,
        grid=(length // block,),
        out_shape=[whole, whole, jax.ShapeDtypeStruct((8, length), f32), jax.ShapeDtypeStruct((16, 128), f32)],
        in_specs=[columns] * 4 + [pl.BlockSpec((8, 128), lambda i: (0, 0))] + [pl.BlockSpec(memory_space=pl.ANY)] * len(before),
        out_specs=[columns, columns, pl.BlockSpec((8, block), lambda i: (0, i)), pl.BlockSpec((16, 128), lambda i: (0, 0))],
        input_output_aliases={5 + index: index for index in range(len(before))},
        cost_estimate=pl.CostEstimate(flops=bytes_moved, bytes_accessed=bytes_moved, transcendentals=0),
        compiler_params=pltpu.CompilerParams(dimension_semantics=("arbitrary",)),
    )(g, w, m, v, total, *before)


def pack(kind, full, packed):
    if kind == 4:
        half = packed.shape[1]
        packed[0:4] = full[0:4, 0:half]
        packed[4:8] = full[0:4, half:]
    if kind == 6:
        quarter = packed.shape[1] // 3
        packed[0:6] = full[0:6, 0:3 * quarter]
        for part in range(3):
            packed[6:8, part * quarter:(part + 1) * quarter] = full[2 * part:2 * part + 2, 3 * quarter:]


def weight_kernel(kind, splits, w, u, ratio, *refs):
    count = len(splits) if splits else 1
    outs = refs[-2 - count:-1]
    new_w, sent, packed = outs[0], outs[1:], refs[-1]
    scale = ratio[...]

    def step(index, carry):
        for part in range(8):
            at = pl.ds(pl.multiple_of(index * 1024 + part * 128, 128), 128)
            new_w[:, at] = w[:, at] - scale * u[:, at]
        return carry

    lax.fori_loop(0, w.shape[1] // 1024, step, 0)
    if kind == 8:
        sent[0][...] = new_w[...].astype(jnp.bfloat16)
        return
    pack(kind, new_w, packed)
    if count == 1:
        sent[0][...] = packed[...].astype(jnp.bfloat16)
        return
    start = 0
    i = pl.program_id(0)
    for index, size in enumerate(splits):
        @pl.when(jnp.logical_and(i >= start, i < start + size))
        def _():
            sent[index][...] = packed[...].astype(jnp.bfloat16)
        start += size


def new_weights(name, row_block, kind, block, w, u, ratio, splits=None, before=()):
    rows, length = w.shape
    columns = pl.BlockSpec((8, block), lambda i: (row_block, i))
    width = block * kind // 8
    parts = splits or (length // block,)
    starts = [sum(parts[:index]) for index in range(len(parts))]
    bytes_moved = 8 * length * 4 * 4
    return pl.pallas_call(
        functools.partial(weight_kernel, kind, splits),
        name=name,
        grid=(length // block,),
        out_shape=[jax.ShapeDtypeStruct((rows, length), jnp.float32)] + [jax.ShapeDtypeStruct((8, width * part), jnp.bfloat16) for part in parts],
        in_specs=[columns, pl.BlockSpec((8, block), lambda i: (0, i)), pl.BlockSpec((8, 128), lambda i: (0, 0))]
        + [pl.BlockSpec(memory_space=pl.ANY)] * len(before),
        out_specs=[columns] + [pl.BlockSpec((8, width), lambda i, start=start, part=part: (0, jnp.clip(i - start, 0, part - 1))) for start, part in zip(starts, parts)],
        scratch_shapes=[pltpu.VMEM((8, width), jnp.float32)],
        input_output_aliases={3: 0} if before else {},
        cost_estimate=pl.CostEstimate(flops=bytes_moved, bytes_accessed=bytes_moved, transcendentals=0),
        compiler_params=pltpu.CompilerParams(dimension_semantics=("arbitrary",)),
    )(w, u, ratio, *before)


def unpack_attn_kernel(low, high, out):
    half = high.shape[2]
    out[0:8] = low[0]
    rest = high[0].astype(jnp.float32)
    out[8:12, 0:half] = rest[0:4].astype(jnp.bfloat16)
    out[8:12, half:] = rest[4:8].astype(jnp.bfloat16)


def unpack_attn(low, high, block):
    devices, _, length = low.shape
    blocks = length // block
    bytes_moved = devices * length * 12 * 4
    return pl.pallas_call(
        unpack_attn_kernel,
        name="unpack_attn",
        grid=(devices, blocks),
        out_shape=jax.ShapeDtypeStruct((12, devices * length), jnp.bfloat16),
        in_specs=[pl.BlockSpec((1, 8, block), lambda d, i: (d, 0, i)), pl.BlockSpec((1, 8, block // 2), lambda d, i: (d, 0, i))],
        out_specs=pl.BlockSpec((12, block), lambda d, i: (0, d * blocks + i)),
        cost_estimate=pl.CostEstimate(flops=bytes_moved, bytes_accessed=bytes_moved, transcendentals=0),
        compiler_params=pltpu.CompilerParams(dimension_semantics=("arbitrary", "arbitrary")),
    )(low, high)


def unpack_mlp_kernel(packed, *refs):
    out = refs[-1]
    quarter = packed.shape[2] // 3
    full = packed[0].astype(jnp.float32)
    out[:, 0:3 * quarter] = full[0:6].astype(jnp.bfloat16)
    for part in range(3):
        out[2 * part:2 * part + 2, 3 * quarter:] = full[6:8, part * quarter:(part + 1) * quarter].astype(jnp.bfloat16)


def unpack_mlp(packed, block, start, blocks, before):
    devices = packed.shape[0]
    width = block * 6 // 8
    count = packed.shape[2] // width
    bytes_moved = packed.size * 4
    return pl.pallas_call(
        unpack_mlp_kernel,
        name=f"unpack_mlp_{start}",
        grid=(devices, count),
        out_shape=jax.ShapeDtypeStruct((6, devices * blocks * block), jnp.bfloat16),
        in_specs=[pl.BlockSpec((1, 8, width), lambda d, i: (d, 0, i))] + [pl.BlockSpec(memory_space=pl.ANY)] * len(before),
        out_specs=pl.BlockSpec((6, block), lambda d, i: (0, d * blocks + start + i)),
        input_output_aliases={1: 0} if before else {},
        cost_estimate=pl.CostEstimate(flops=bytes_moved, bytes_accessed=bytes_moved, transcendentals=0),
        compiler_params=pltpu.CompilerParams(dimension_semantics=("arbitrary", "arbitrary")),
    )(packed, *before)


def solution(mesh):
    group_size = mesh.shape["data"]
    grad_spec = P("data", None, None)
    shard_spec = P(None, "data")
    full_spec = P(None, None)

    def local_step(*all_banks):
        weights = all_banks[4:8]
        firsts = all_banks[8:12]
        seconds = all_banks[12:16]
        *mean_grads, total = reduce_scatter(group_size, *all_banks[0:4])

        state = [(mean_grads[bank], weights[bank], firsts[bank], seconds[bank], total) for bank in range(2)]
        attn_m, attn_v, u, norms = moments("moments_high", 1, 4, ATTN_BLOCK, *state[0])
        ratio = sum_over_devices(group_size, norms, "share_high", 1, True)
        attn_w, sent = new_weights("weights_high", 1, 4, ATTN_BLOCK, weights[0], u, ratio)
        high = lax.all_gather(sent, "data")

        attn_m, attn_v, u, norms = moments("moments_low", 0, 8, ATTN_BLOCK, *state[0], before=(attn_m, attn_v))
        ratio = sum_over_devices(group_size, norms, "share_low", 2, True)
        attn_w, sent = new_weights("weights_low", 0, 8, ATTN_BLOCK, weights[0], u, ratio, before=(attn_w,))
        low = lax.all_gather(sent, "data")

        mlp_m, mlp_v, u, norms = moments("moments_mlp", 0, 6, MLP_BLOCK, *state[1])
        ratio = sum_over_devices(group_size, norms, "share_mlp", 3, True)
        mlp_w, *sent = new_weights("weights_mlp", 0, 6, MLP_BLOCK, weights[1], u, ratio, splits=MLP_SPLITS)
        gathered = [lax.all_gather(part, "data") for part in sent]

        clip_coef = jnp.minimum(1.0, MAX_NORM / jnp.sqrt(total[0, 0]))
        results = [adam_direction(mean_grads[bank], weights[bank], firsts[bank], seconds[bank], clip_coef) for bank in (2, 3)]
        part_sums = jnp.concatenate([jnp.sum(weight * weight, axis=1) for weight in weights[2:]] + [jnp.sum(result[0] * result[0], axis=1) for result in results])
        count = part_sums.shape[0]
        tile = jnp.pad(part_sums, (0, 1024 - count)).reshape(8, 128)
        norm_sums = sum_over_devices(group_size, tile, "share_small", 4, False).reshape(1024)[:count]
        trust_ratios = jnp.sqrt(norm_sums[:count // 2]) / jnp.sqrt(norm_sums[count // 2:])
        small_replicas, small_weights = [], []
        first_row = 0
        for index in range(2):
            weight = weights[2 + index]
            row_count = weight.shape[0]
            trust_ratio = trust_ratios[first_row:first_row + row_count]
            first_row = first_row + row_count
            new_weight = weight - LEARN_RATE * trust_ratio[:, None] * results[index][0]
            small_weights.append(new_weight)
            small_replicas.append(lax.all_gather(new_weight.astype(jnp.bfloat16), "data", axis=1, tiled=True))

        attn_replica = unpack_attn(low, high, ATTN_BLOCK)
        blocks = weights[1].shape[1] // MLP_BLOCK
        mlp_replica = ()
        start = 0
        for part, size in zip(gathered, MLP_SPLITS):
            mlp_replica = (unpack_mlp(part, MLP_BLOCK, start, blocks, mlp_replica),)
            start += size
        return (attn_replica, *mlp_replica, *small_replicas, attn_w, mlp_w, *small_weights,
                attn_m, mlp_m, results[0][1], results[1][1], attn_v, mlp_v, results[0][2], results[1][2])

    return jax.shard_map(local_step, mesh=mesh, in_specs=(grad_spec,) * 4 + (shard_spec,) * 12, out_specs=(full_spec,) * 4 + (shard_spec,) * 12, check_vma=False)
```

```python
import functools

import jax
import jax.numpy as jnp
from jax import lax
from jax.experimental import pallas as pl
from jax.experimental.pallas import tpu as pltpu
from jax.sharding import PartitionSpec as P

STEP_NUMBER = 10
LEARN_RATE = 0.04
BETA_FIRST = 0.9
BETA_SECOND = 0.999
EPSILON = 1e-6
WEIGHT_DECAY = 0.01
MAX_NORM = 1.0
FIRST_SCALE = 1.0 / (1.0 - BETA_FIRST ** STEP_NUMBER)
SECOND_SCALE = 1.0 / (1.0 - BETA_SECOND ** STEP_NUMBER)


MESH = pl.DeviceIdType.MESH
SLOTS = 8
AHEAD = 2
LAG_ONE = 4
LAG_TWO = 8
WIDTH = 1024
OUT_SLOTS = 4
ATTN_BLOCK = 16384
MLP_BLOCK = 16384
MLP_SPLITS = (12, 12, 8)


def signal_all_and_wait(me, devices):
    barrier = pltpu.get_barrier_semaphore()
    for step in range(1, devices):
        pl.semaphore_signal(barrier, inc=1, device_id=(lax.rem(me + step, devices),), device_id_type=MESH)
    pl.semaphore_wait(barrier, devices - 1)


def share_tile(me, devices, tiles, send_sem, recv_sem):
    copies = []
    for step in range(1, devices):
        other = lax.rem(me + step, devices)
        copy = pltpu.make_async_remote_copy(
            src_ref=tiles.at[me], dst_ref=tiles.at[me], send_sem=send_sem.at[step], recv_sem=recv_sem.at[step],
            device_id=(other,), device_id_type=MESH)
        copy.start()
        copies.append(copy)
    for copy in copies:
        copy.wait()


def pieces(width):
    half, three = width // 2, 3 * width
    first = width + half
    attn, mlp = range(2)
    low, high, right = slice(8), slice(8, None), slice(width, first)
    table = [
        (attn, (low, slice(width)), (low, slice(width))),
        (attn, (high, slice(half)), (slice(4), right)),
        (attn, (high, slice(half, width)), (slice(4, 8), right)),
        (mlp, (slice(6), slice(three)), (slice(6), slice(first, first + three))),
    ]
    for part in range(3):
        start = first + part * width
        table.append((mlp, (slice(2 * part, 2 * part + 2), slice(three, None)), (slice(6, 8), slice(start, start + width))))
    return table


def scatter_kernel(devices, width, chunks, ga, gm, gw, gv, oa, om, ow, ov, total,
                   la, lm, pa, pm, s1, r1, s2, r2, staged, ua, um, rw, rv, sq, tiles,
                   load_sem, psend_sem, precv_sem, out_sem, send1_sem, recv1_sem, send2_sem, recv2_sem,
                   wsend_sem, wrecv_sem, vsend_sem, vrecv_sem, tsend_sem, trecv_sem, pcredit, credit1, credit2):
    me = lax.axis_index("data")
    core = lax.rem(me, 2)
    x = lax.rem(me // 2, 2)
    y = me // 4
    partner = me + 1 - 2 * core
    xn = y * 4 + (1 - x) * 2 + core
    yn = (1 - y) * 4 + x * 2 + core
    banks = ((ga, oa, la, pa, ua, width), (gm, om, lm, pm, um, 4 * width))

    signal_all_and_wait(me, devices)

    small = []
    for step in range(1, devices):
        other = lax.rem(me + step, devices)
        for src, dst, ssem, rsem in ((gw, rw, wsend_sem, wrecv_sem), (gv, rv, vsend_sem, vrecv_sem)):
            small_width = dst.shape[2]
            copy = pltpu.make_async_remote_copy(
                src_ref=src.at[0, :, pl.ds(pl.multiple_of(other * small_width, small_width), small_width)], dst_ref=dst.at[step],
                send_sem=ssem.at[step], recv_sem=rsem.at[step], device_id=(other,), device_id_type=MESH)
            copy.start()
            small.append(copy)

    sq[...] = jnp.zeros_like(sq)

    def chips(kind):
        fx, fy = x + kind * (1 - 2 * x), y + (1 - kind) * (1 - 2 * y)
        nx, ny = x + (1 - kind) * (1 - 2 * x), y + kind * (1 - 2 * y)
        return ((x, y), (fx, fy), (nx, ny), (1 - x, 1 - y))

    def first_peer(kind):
        return xn + kind * (yn - xn)

    def second_peer(kind):
        return yn + kind * (xn - yn)

    def send_one(slot, kind):
        return pltpu.make_async_remote_copy(
            src_ref=s1.at[slot], dst_ref=r1.at[slot], send_sem=send1_sem.at[slot], recv_sem=recv1_sem.at[slot],
            device_id=(first_peer(kind),), device_id_type=MESH)

    def send_two(slot, kind):
        return pltpu.make_async_remote_copy(
            src_ref=s2.at[slot], dst_ref=r2.at[slot], send_sem=send2_sem.at[slot], recv_sem=recv2_sem.at[slot],
            device_id=(second_peer(kind),), device_id_type=MESH)

    def out_copy(chunk, bank):
        out, unpacked, columns = banks[bank][1], banks[bank][4], banks[bank][5]
        slot = lax.rem(chunk, OUT_SLOTS)
        return pltpu.make_async_copy(unpacked.at[slot], out.at[:, pl.ds(pl.multiple_of(chunk * columns, columns), columns)], out_sem.at[bank, slot])

    def pair_sums(slot, block):
        return [banks[bank][2][slot, block].astype(jnp.float32) + banks[bank][3][slot, block].astype(jnp.float32) for bank in range(2)]

    def body(i, carry):
        d = i - AHEAD - LAG_TWO

        @pl.when(d >= 0)
        def _():
            slot = lax.rem(d, SLOTS)
            kind = lax.rem(d, 2)
            send_two(slot, kind).wait_recv()

            @pl.when(d >= OUT_SLOTS)
            def _():
                for bank in range(2):
                    out_copy(d - OUT_SLOTS, bank).wait()

            square = sq[...]
            for at in range(0, s2.shape[2], 128):
                mean = (staged[slot, :, at:at + 128] + r2[slot, :, at:at + 128]) * (1.0 / devices)
                staged[slot, :, at:at + 128] = mean
                square = square + mean * mean
            sq[...] = square
            out_slot = lax.rem(d, OUT_SLOTS)
            for bank, place, packed in pieces(width):
                banks[bank][4][(out_slot, *place)] = staged[(slot, *packed)]
            for bank in range(2):
                out_copy(d, bank).start()

            @pl.when(d + SLOTS < chunks)
            def _():
                pl.semaphore_signal(credit2.at[kind], inc=1, device_id=(second_peer(kind),), device_id_type=MESH)

            send_one(slot, kind).wait_send()
            send_two(slot, kind).wait_send()

        c = i - AHEAD - LAG_ONE

        @pl.when(jnp.logical_and(c >= 0, c < chunks))
        def _():
            slot = lax.rem(c, SLOTS)
            kind = lax.rem(c, 2)

            @pl.when(c >= SLOTS)
            def _():
                pl.semaphore_wait(credit2.at[kind], 1)

            send_one(slot, kind).wait_recv()
            sums = pair_sums(slot, 1)
            for bank, place, packed in pieces(width):
                s2[(slot, *packed)] = r1[(slot, 1, *packed)] + sums[bank][place]
            send_two(slot, kind).start()
            sums = pair_sums(slot, 0)
            for bank, place, packed in pieces(width):
                staged[(slot, *packed)] = r1[(slot, 0, *packed)] + sums[bank][place]

            @pl.when(c + SLOTS < chunks)
            def _():
                pl.semaphore_signal(pcredit, inc=1, device_id=(partner,), device_id_type=MESH)
                pl.semaphore_signal(credit1.at[kind], inc=1, device_id=(first_peer(kind),), device_id_type=MESH)

            for bank in range(2):
                p = banks[bank][3]
                pltpu.make_async_copy(p.at[slot], p.at[slot], psend_sem.at[bank, slot]).wait()

        b = i - AHEAD

        @pl.when(jnp.logical_and(b >= 0, b < chunks))
        def _():
            slot = lax.rem(b, SLOTS)
            kind = lax.rem(b, 2)

            @pl.when(b >= SLOTS)
            def _():
                pl.semaphore_wait(credit1.at[kind], 1)

            for bank in range(2):
                l, p = banks[bank][2], banks[bank][3]
                pltpu.make_async_copy(l.at[slot], l.at[slot], load_sem.at[bank, slot]).wait()
                pltpu.make_async_copy(p.at[slot], p.at[slot], precv_sem.at[bank, slot]).wait()
            for block in range(2):
                sums = pair_sums(slot, 2 + block)
                for bank, place, packed in pieces(width):
                    s1[(slot, block, *packed)] = sums[bank][place]
            send_one(slot, kind).start()

        @pl.when(i < chunks)
        def _():
            slot = lax.rem(i, SLOTS)
            kind = lax.rem(i, 2)

            @pl.when(i >= SLOTS)
            def _():
                pl.semaphore_wait(pcredit, 1)

            for bank in range(2):
                g, l, p, columns = banks[bank][0], banks[bank][2], banks[bank][3], banks[bank][5]
                length = g.shape[2] // devices
                for block, (bx, by) in enumerate(chips(kind)):
                    chip = by * 4 + bx * 2
                    theirs = pl.multiple_of((chip + 1 - core) * length + i * columns, columns)
                    pltpu.make_async_remote_copy(
                        src_ref=g.at[0, :, pl.ds(theirs, columns)], dst_ref=p.at[slot, block],
                        send_sem=psend_sem.at[bank, slot], recv_sem=precv_sem.at[bank, slot],
                        device_id=(partner,), device_id_type=MESH).start()
                    mine = pl.multiple_of((chip + core) * length + i * columns, columns)
                    pltpu.make_async_copy(g.at[0, :, pl.ds(mine, columns)], l.at[slot, block], load_sem.at[bank, slot]).start()

        return carry

    lax.fori_loop(0, chunks + AHEAD + LAG_TWO, body, 0)

    for copy in small:
        copy.wait()
    square = jnp.sum(sq[...], axis=0, keepdims=True)
    for src, received, out in ((gw, rw, ow), (gv, rv, ov)):
        small_width = received.shape[2]
        mean = src[0, :, pl.ds(pl.multiple_of(me * small_width, small_width), small_width)].astype(jnp.float32)
        for step in range(1, devices):
            mean = mean + received[step].astype(jnp.float32)
        mean = mean * (1.0 / devices)
        out[...] = mean
        for at in range(0, small_width, 128):
            part = mean[:, at:at + 128]
            square = square + jnp.sum(part * part, axis=0, keepdims=True)
    tiles[me] = jnp.broadcast_to(square, tiles.shape[1:])
    share_tile(me, devices, tiles, tsend_sem, trecv_sem)
    everything = tiles[0]
    for device in range(1, devices):
        everything = everything + tiles[device]
    total[...] = jnp.broadcast_to(jnp.sum(everything[0:1], axis=1, keepdims=True), total.shape)

    for chunk in range(chunks - OUT_SLOTS, chunks):
        for bank in range(2):
            out_copy(chunk, bank).wait()


def reduce_scatter(devices, ga, gm, gw, gv):
    f32, bf16 = jnp.float32, jnp.bfloat16
    rows = (ga.shape[1], gm.shape[1])
    lengths = (ga.shape[2] // devices, gm.shape[2] // devices)
    chunks = lengths[0] // WIDTH
    widths = (WIDTH, lengths[1] // chunks)
    small = (gw.shape[2] // devices, gv.shape[2] // devices)
    packed = (rows[0] * widths[0] + rows[1] * widths[1]) // 8

    def unpacked(lead, dtype):
        return [pltpu.VMEM(lead + (rows[bank], widths[bank]), dtype) for bank in range(2)]

    dma = pltpu.SemaphoreType.DMA
    scratch = (
        unpacked((SLOTS, 4), bf16) + unpacked((SLOTS, 4), bf16)
        + [pltpu.VMEM((SLOTS, 2, 8, packed), f32)] * 2 + [pltpu.VMEM((SLOTS, 8, packed), f32)] * 3
        + unpacked((OUT_SLOTS,), f32)
        + [pltpu.VMEM((devices, gw.shape[1], small[0]), bf16), pltpu.VMEM((devices, gv.shape[1], small[1]), bf16)]
        + [pltpu.VMEM((8, 128), f32), pltpu.VMEM((devices, 8, 128), f32)]
        + [dma((2, SLOTS))] * 3 + [dma((2, OUT_SLOTS))] + [dma((SLOTS,))] * 4 + [dma((devices,))] * 6
        + [pltpu.SemaphoreType.REGULAR, pltpu.SemaphoreType.REGULAR((2,)), pltpu.SemaphoreType.REGULAR((2,))]
    )
    vmem = pl.BlockSpec(memory_space=pltpu.VMEM)
    anywhere = pl.BlockSpec(memory_space=pl.ANY)
    return pl.pallas_call(
        functools.partial(scatter_kernel, devices, WIDTH, chunks),
        name="scatter",
        out_shape=[jax.ShapeDtypeStruct((rows[0], lengths[0]), f32), jax.ShapeDtypeStruct((rows[1], lengths[1]), f32),
                   jax.ShapeDtypeStruct((gw.shape[1], small[0]), f32), jax.ShapeDtypeStruct((gv.shape[1], small[1]), f32),
                   jax.ShapeDtypeStruct((8, 128), f32)],
        in_specs=[anywhere, anywhere, vmem, vmem],
        out_specs=[anywhere, anywhere, vmem, vmem, vmem],
        scratch_shapes=scratch,
        compiler_params=pltpu.CompilerParams(collective_id=0, has_side_effects=True, vmem_limit_bytes=48 * 1024 * 1024),
    )(ga, gm, gw, gv)


def adam_direction(mean_grad, weight, first_moment, second_moment, clip_coef):
    clipped = clip_coef * mean_grad
    new_first = BETA_FIRST * first_moment + (1.0 - BETA_FIRST) * clipped
    new_second = BETA_SECOND * second_moment + (1.0 - BETA_SECOND) * (clipped * clipped)
    update = (new_first * FIRST_SCALE) / (jnp.sqrt(new_second * SECOND_SCALE) + EPSILON) + WEIGHT_DECAY * weight
    return update, new_first, new_second


def share_kernel(devices, part, total, tiles, send_sem, recv_sem):
    me = lax.axis_index("data")
    signal_all_and_wait(me, devices)
    tiles[me] = part[...]
    share_tile(me, devices, tiles, send_sem, recv_sem)
    everything = tiles[0]
    for device in range(1, devices):
        everything = everything + tiles[device]
    if total.shape == part.shape:
        total[...] = everything
    else:
        weight_norm = jnp.sqrt(jnp.sum(everything[0:8], axis=1, keepdims=True))
        update_norm = jnp.sqrt(jnp.sum(everything[8:16], axis=1, keepdims=True))
        total[...] = jnp.broadcast_to(LEARN_RATE * (weight_norm / update_norm), total.shape)


def sum_over_devices(devices, part, name, collective_id, ratio):
    dma = pltpu.SemaphoreType.DMA
    vmem = pl.BlockSpec(memory_space=pltpu.VMEM)
    return pl.pallas_call(
        functools.partial(share_kernel, devices),
        name=name,
        out_shape=jax.ShapeDtypeStruct((8, 128) if ratio else part.shape, part.dtype),
        in_specs=[vmem],
        out_specs=vmem,
        scratch_shapes=[pltpu.VMEM((devices,) + part.shape, part.dtype), dma((devices,)), dma((devices,))],
        compiler_params=pltpu.CompilerParams(collective_id=collective_id, has_side_effects=True),
    )(part)


def moment_kernel(valid, g, w, m, v, total, *refs):
    new_m, new_v, u, norms = refs[-4:]
    clip = jnp.minimum(1.0, MAX_NORM / jnp.sqrt(total[...]))

    @pl.when(pl.program_id(0) == 0)
    def _():
        norms[...] = jnp.zeros_like(norms)

    def step(index, carry):
        weight_square, update_square = carry
        for part in range(8):
            at = pl.ds(pl.multiple_of(index * 1024 + part * 128, 128), 128)
            weight = w[:, at]
            update, first, second = adam_direction(g[:, at], weight, m[:, at], v[:, at], clip)
            new_m[:, at] = first
            new_v[:, at] = second
            u[:, at] = update
            weight_square = weight_square + weight * weight
            update_square = update_square + update * update
        return weight_square, update_square

    zero = jnp.zeros((8, 128), jnp.float32)
    weight_square, update_square = lax.fori_loop(0, g.shape[1] // 1024, step, (zero, zero))
    row = lax.broadcasted_iota(jnp.int32, (8, 128), 0)
    norms[0:8] += jnp.where(row < valid, weight_square, 0.0)
    norms[8:16] += jnp.where(row < valid, update_square, 0.0)


def moments(name, row_block, valid, block, g, w, m, v, total, before=()):
    f32 = jnp.float32
    rows, length = g.shape
    columns = pl.BlockSpec((8, block), lambda i: (row_block, i))
    whole = jax.ShapeDtypeStruct((rows, length), f32)
    bytes_moved = 8 * length * 4 * 7
    return pl.pallas_call(
        functools.partial(moment_kernel, valid),
        name=name,
        grid=(length // block,),
        out_shape=[whole, whole, jax.ShapeDtypeStruct((8, length), f32), jax.ShapeDtypeStruct((16, 128), f32)],
        in_specs=[columns] * 4 + [pl.BlockSpec((8, 128), lambda i: (0, 0))] + [pl.BlockSpec(memory_space=pl.ANY)] * len(before),
        out_specs=[columns, columns, pl.BlockSpec((8, block), lambda i: (0, i)), pl.BlockSpec((16, 128), lambda i: (0, 0))],
        input_output_aliases={5 + index: index for index in range(len(before))},
        cost_estimate=pl.CostEstimate(flops=bytes_moved, bytes_accessed=bytes_moved, transcendentals=0),
        compiler_params=pltpu.CompilerParams(dimension_semantics=("arbitrary",)),
    )(g, w, m, v, total, *before)


def pack(kind, full, packed):
    if kind == 4:
        half = packed.shape[1]
        packed[0:4] = full[0:4, 0:half]
        packed[4:8] = full[0:4, half:]
    if kind == 6:
        quarter = packed.shape[1] // 3
        packed[0:6] = full[0:6, 0:3 * quarter]
        for part in range(3):
            packed[6:8, part * quarter:(part + 1) * quarter] = full[2 * part:2 * part + 2, 3 * quarter:]


def weight_kernel(kind, splits, w, u, ratio, *refs):
    count = len(splits) if splits else 1
    outs = refs[-2 - count:-1]
    new_w, sent, packed = outs[0], outs[1:], refs[-1]
    scale = ratio[...]

    def step(index, carry):
        for part in range(8):
            at = pl.ds(pl.multiple_of(index * 1024 + part * 128, 128), 128)
            new_w[:, at] = w[:, at] - scale * u[:, at]
        return carry

    lax.fori_loop(0, w.shape[1] // 1024, step, 0)
    if kind == 8:
        sent[0][...] = new_w[...].astype(jnp.bfloat16)
        return
    pack(kind, new_w, packed)
    if count == 1:
        sent[0][...] = packed[...].astype(jnp.bfloat16)
        return
    start = 0
    i = pl.program_id(0)
    for index, size in enumerate(splits):
        @pl.when(jnp.logical_and(i >= start, i < start + size))
        def _():
            sent[index][...] = packed[...].astype(jnp.bfloat16)
        start += size


def new_weights(name, row_block, kind, block, w, u, ratio, splits=None, before=()):
    rows, length = w.shape
    columns = pl.BlockSpec((8, block), lambda i: (row_block, i))
    width = block * kind // 8
    parts = splits or (length // block,)
    starts = [sum(parts[:index]) for index in range(len(parts))]
    bytes_moved = 8 * length * 4 * 4
    return pl.pallas_call(
        functools.partial(weight_kernel, kind, splits),
        name=name,
        grid=(length // block,),
        out_shape=[jax.ShapeDtypeStruct((rows, length), jnp.float32)] + [jax.ShapeDtypeStruct((8, width * part), jnp.bfloat16) for part in parts],
        in_specs=[columns, pl.BlockSpec((8, block), lambda i: (0, i)), pl.BlockSpec((8, 128), lambda i: (0, 0))]
        + [pl.BlockSpec(memory_space=pl.ANY)] * len(before),
        out_specs=[columns] + [pl.BlockSpec((8, width), lambda i, start=start, part=part: (0, jnp.clip(i - start, 0, part - 1))) for start, part in zip(starts, parts)],
        scratch_shapes=[pltpu.VMEM((8, width), jnp.float32)],
        input_output_aliases={3: 0} if before else {},
        cost_estimate=pl.CostEstimate(flops=bytes_moved, bytes_accessed=bytes_moved, transcendentals=0),
        compiler_params=pltpu.CompilerParams(dimension_semantics=("arbitrary",)),
    )(w, u, ratio, *before)


def unpack_rows(kind, packed, out):
    if kind == 8:
        out[0:8] = packed[...]
    if kind == 4:
        half = packed.shape[1]
        out[8:12, 0:half] = packed[0:4]
        out[8:12, half:] = packed[4:8]
    if kind == 6:
        quarter = packed.shape[1] // 3
        out[:, 0:3 * quarter] = packed[0:6]
        for part in range(3):
            out[2 * part:2 * part + 2, 3 * quarter:] = packed[6:8, part * quarter:(part + 1) * quarter]


def unpack_kernel(kinds, devices, owners, *refs):
    out = refs[-1]
    for source in range(devices):
        @pl.when(pl.program_id(0) == source)
        def _():
            for index, kind in enumerate(kinds):
                unpack_rows(kind, refs[index * devices + source], out)


def unpack(name, kinds, sources, owners, rows, block, start, blocks, before=()):
    devices = owners.shape[0]
    count = sources[0][0].shape[1] * 8 // (block * kinds[0])

    def spec(kind, source):
        def index(d, i, owners):
            return 0, jnp.where(d < source, 0, jnp.where(d == source, i, count - 1))
        return pl.BlockSpec((8, block * kind // 8), index)

    bytes_moved = devices * count * block * rows * 4
    arrays = [array for group in sources for array in group]
    return pl.pallas_call(
        functools.partial(unpack_kernel, kinds, devices),
        name=name,
        grid_spec=pltpu.PrefetchScalarGridSpec(
            num_scalar_prefetch=1,
            grid=(devices, count),
            in_specs=[spec(kind, source) for kind in kinds for source in range(devices)] + [pl.BlockSpec(memory_space=pl.ANY)] * len(before),
            out_specs=pl.BlockSpec((rows, block), lambda d, i, owners: (0, owners[d] * blocks + start + i))),
        out_shape=jax.ShapeDtypeStruct((rows, devices * blocks * block), jnp.bfloat16),
        input_output_aliases={1 + len(arrays): 0} if before else {},
        cost_estimate=pl.CostEstimate(flops=bytes_moved, bytes_accessed=bytes_moved, transcendentals=0),
        compiler_params=pltpu.CompilerParams(dimension_semantics=("arbitrary", "arbitrary")),
    )(owners, *arrays, *before)


def exchange(array, bit, devices):
    return lax.ppermute(array, "data", [(device, device ^ bit) for device in range(devices)])


def gather(sent, turn, devices):
    from_x = exchange(sent, 2, devices)
    from_y = exchange(sent, 4, devices)
    from_diagonal = exchange(from_y, 2, devices) if turn else exchange(from_x, 4, devices)
    near = [sent, from_x, from_y, from_diagonal]
    return near + [exchange(array, 1, devices) for array in near]


def solution(mesh):
    group_size = mesh.shape["data"]
    grad_spec = P("data", None, None)
    shard_spec = P(None, "data")
    full_spec = P(None, None)

    def local_step(*all_banks):
        weights = all_banks[4:8]
        firsts = all_banks[8:12]
        seconds = all_banks[12:16]
        *mean_grads, total = reduce_scatter(group_size, *all_banks[0:4])

        state = [(mean_grads[bank], weights[bank], firsts[bank], seconds[bank], total) for bank in range(2)]
        attn_m, attn_v, u, norms = moments("moments_high", 1, 4, ATTN_BLOCK, *state[0])
        ratio = sum_over_devices(group_size, norms, "share_high", 1, True)
        attn_w, sent = new_weights("weights_high", 1, 4, ATTN_BLOCK, weights[0], u, ratio)
        high = gather(sent, 0, group_size)

        attn_m, attn_v, u, norms = moments("moments_low", 0, 8, ATTN_BLOCK, *state[0], before=(attn_m, attn_v))
        ratio = sum_over_devices(group_size, norms, "share_low", 2, True)
        attn_w, sent = new_weights("weights_low", 0, 8, ATTN_BLOCK, weights[0], u, ratio, before=(attn_w,))
        low = gather(sent, 1, group_size)

        mlp_m, mlp_v, u, norms = moments("moments_mlp", 0, 6, MLP_BLOCK, *state[1])
        ratio = sum_over_devices(group_size, norms, "share_mlp", 3, True)
        mlp_w, *sent = new_weights("weights_mlp", 0, 6, MLP_BLOCK, weights[1], u, ratio, splits=MLP_SPLITS)
        gathered = [gather(part, index % 2, group_size) for index, part in enumerate(sent)]

        clip_coef = jnp.minimum(1.0, MAX_NORM / jnp.sqrt(total[0, 0]))
        results = [adam_direction(mean_grads[bank], weights[bank], firsts[bank], seconds[bank], clip_coef) for bank in (2, 3)]
        part_sums = jnp.concatenate([jnp.sum(weight * weight, axis=1) for weight in weights[2:]] + [jnp.sum(result[0] * result[0], axis=1) for result in results])
        count = part_sums.shape[0]
        tile = jnp.pad(part_sums, (0, 1024 - count)).reshape(8, 128)
        norm_sums = sum_over_devices(group_size, tile, "share_small", 4, False).reshape(1024)[:count]
        trust_ratios = jnp.sqrt(norm_sums[:count // 2]) / jnp.sqrt(norm_sums[count // 2:])
        small_replicas, small_weights = [], []
        first_row = 0
        for index in range(2):
            weight = weights[2 + index]
            row_count = weight.shape[0]
            trust_ratio = trust_ratios[first_row:first_row + row_count]
            first_row = first_row + row_count
            new_weight = weight - LEARN_RATE * trust_ratio[:, None] * results[index][0]
            small_weights.append(new_weight)
            small_replicas.append(lax.all_gather(new_weight.astype(jnp.bfloat16), "data", axis=1, tiled=True))

        owners = jnp.bitwise_xor(lax.axis_index("data"), jnp.array([0, 2, 4, 6, 1, 3, 5, 7], jnp.int32))
        blocks = weights[0].shape[1] // ATTN_BLOCK
        attn_replica = unpack("unpack_attn", (8, 4), (low, high), owners, 12, ATTN_BLOCK, 0, blocks)
        blocks = weights[1].shape[1] // MLP_BLOCK
        mlp_replica = ()
        start = 0
        for part, size in zip(gathered, MLP_SPLITS):
            mlp_replica = (unpack(f"unpack_mlp_{start}", (6,), (part,), owners, 6, MLP_BLOCK, start, blocks, mlp_replica),)
            start += size
        return (attn_replica, *mlp_replica, *small_replicas, attn_w, mlp_w, *small_weights,
                attn_m, mlp_m, results[0][1], results[1][1], attn_v, mlp_v, results[0][2], results[1][2])

    return jax.shard_map(local_step, mesh=mesh, in_specs=(grad_spec,) * 4 + (shard_spec,) * 12, out_specs=(full_spec,) * 4 + (shard_spec,) * 12, check_vma=False)
```
